32 devices in a mesh: pod: 8 (over z, y), data: 4 (over x, core).
Axes of the slice: x: 2, y: 2, z: 4, core: 2. Of those that a mesh axis runs over, the one named last changes fastest.
Arguments:
- w_first: float32 [12, 512, 2048], replicated
- w_second: float32 [12, 2048, 512], replicated
- m_first: float32 [12, 512, 2048], replicated
- m_second: float32 [12, 2048, 512], replicated
- x_now: bfloat16 [16384, 512], P(('pod', 'data'))
- y_now: bfloat16 [16384, 512], P(('pod', 'data'))
- x_next: bfloat16 [16384, 512], P(('pod', 'data'))
- y_next: bfloat16 [16384, 512], P(('pod', 'data'))
Outputs:
- output 1: float32 [12, 512, 2048], replicated
- output 2: float32 [12, 2048, 512], replicated
- output 3: float32 [12, 512, 2048], replicated
- output 4: float32 [12, 2048, 512], replicated
- output 5: float32 [16384], P(('pod', 'data'))
- output 6: float32 [16384, 512], P(('pod', 'data'))
All inputs are finite; a program needn't handle non-finite values.
Results may differ from the reference program's by a relative error of at most 0.0107373.
Values are sent between devices in bfloat16 or wider.
A program may use at most 1.75 GiB of HBM per device.

```python
import jax
import jax.numpy as jnp
from jax import lax

D = 512
F = 2048
LAYERS = 12
TOK = 512
DEVICES = 32
BATCH = TOK * DEVICES
LEARN_RATE = 0.25 / LAYERS
MOMENTUM = 0.9
BRANCH_SCALE = (4.0 / max(LAYERS, 4)) ** 0.5


def draw_batch(key_list):
    noise_val = jax.random.normal(key_list[0], (DEVICES, TOK, D), jnp.float32)
    global_off = jax.random.normal(key_list[1], (1, 1, D), jnp.float32)
    device_off = jax.random.normal(key_list[2], (DEVICES, 1, D), jnp.float32)
    rows_val = 0.7 * noise_val + 0.5 * global_off + 0.5 * device_off
    return rows_val.reshape(BATCH, D).astype(jnp.bfloat16)


def setup_inputs(seed: int = 0) -> dict:
    key_list = jax.random.split(jax.random.key(seed), 16)
    w_first = jax.random.normal(key_list[0], (LAYERS, D, F), jnp.float32) * D ** -0.5
    w_second = jax.random.normal(key_list[1], (LAYERS, F, D), jnp.float32) * (F ** -0.5 * BRANCH_SCALE)
    m_first = jax.random.normal(key_list[2], (LAYERS, D, F), jnp.float32) * (0.3 * BRANCH_SCALE / D)
    m_second = jax.random.normal(key_list[3], (LAYERS, F, D), jnp.float32) * (0.7 / D)
    return {'w_first': w_first, 'w_second': w_second, 'm_first': m_first, 'm_second': m_second,
            'x_now': draw_batch(key_list[4:7]), 'y_now': draw_batch(key_list[7:10]),
            'x_next': draw_batch(key_list[10:13]), 'y_next': draw_batch(key_list[13:16])}


def layer_stack(hidden, w_first_low, w_second_low):
    def body(carry, weights):
        pre_act = jnp.dot(carry.astype(jnp.bfloat16), weights[0], preferred_element_type=jnp.float32)
        act_low = jax.nn.gelu(pre_act).astype(jnp.bfloat16)
        return carry + jnp.dot(act_low, weights[1], preferred_element_type=jnp.float32), carry
    return lax.scan(body, hidden, (w_first_low, w_second_low))


def local_grads(rows_in, rows_target, w_first_low, w_second_low):
    h_last, h_saved = layer_stack(rows_in.astype(jnp.float32), w_first_low, w_second_low)
    grad_h = (h_last - rows_target.astype(jnp.float32)) / (BATCH * D)

    def back(grad_carry, layer_item):
        h_in, wf_low, ws_low = layer_item
        h_low = h_in.astype(jnp.bfloat16)
        pre_act = jnp.dot(h_low, wf_low, preferred_element_type=jnp.float32)
        act_val, gelu_back = jax.vjp(jax.nn.gelu, pre_act)
        act_low = act_val.astype(jnp.bfloat16)
        grad_low = grad_carry.astype(jnp.bfloat16)
        g_second = jnp.dot(act_low.T, grad_low, preferred_element_type=jnp.float32)
        grad_act = jnp.dot(grad_low, ws_low.T, preferred_element_type=jnp.float32)
        grad_pre = gelu_back(grad_act)[0].astype(jnp.bfloat16)
        g_first = jnp.dot(h_low.T, grad_pre, preferred_element_type=jnp.float32)
        grad_next = grad_carry + jnp.dot(grad_pre, wf_low.T, preferred_element_type=jnp.float32)
        return grad_next, (g_first.astype(jnp.bfloat16), g_second.astype(jnp.bfloat16))

    return lax.scan(back, grad_h, (h_saved, w_first_low, w_second_low), reverse=True)[1]


def reference(w_first, w_second, m_first, m_second, x_now, y_now, x_next, y_next):
    w_first_low = w_first.astype(jnp.bfloat16)
    w_second_low = w_second.astype(jnp.bfloat16)

    def add_device(grad_acc, rows_pair):
        g_first, g_second = local_grads(rows_pair[0], rows_pair[1], w_first_low, w_second_low)
        return (grad_acc[0] + g_first.astype(jnp.float32), grad_acc[1] + g_second.astype(jnp.float32)), None

    zero_acc = (jnp.zeros(w_first.shape, jnp.float32), jnp.zeros(w_second.shape, jnp.float32))
    rows_now = (x_now.reshape(DEVICES, TOK, D), y_now.reshape(DEVICES, TOK, D))
    (grad_first, grad_second), _ = lax.scan(add_device, zero_acc, rows_now)
    m_first_new = MOMENTUM * m_first + grad_first
    m_second_new = MOMENTUM * m_second + grad_second
    w_first_new = w_first - LEARN_RATE * m_first_new
    w_second_new = w_second - LEARN_RATE * m_second_new
    new_first_low = w_first_new.astype(jnp.bfloat16)
    new_second_low = w_second_new.astype(jnp.bfloat16)

    def next_device(rows_pair):
        h_last = layer_stack(rows_pair[0].astype(jnp.float32), new_first_low, new_second_low)[0]
        resid_rows = h_last - rows_pair[1].astype(jnp.float32)
        return h_last, jnp.sum(resid_rows * resid_rows, axis=-1) / (2 * D)

    rows_next = (x_next.reshape(DEVICES, TOK, D), y_next.reshape(DEVICES, TOK, D))
    h_out, loss_out = lax.map(next_device, rows_next)
    return (w_first_new, w_second_new, m_first_new, m_second_new,
            loss_out.reshape(BATCH), h_out.reshape(BATCH, D))
```

```python
import functools

import jax
import jax.numpy as jnp
from jax import lax
from jax.experimental import pallas as pl
from jax.experimental.pallas import tpu as pltpu
from jax.sharding import PartitionSpec as P

MESH = pl.DeviceIdType.MESH
LEARN_BASE = 0.25
MOMENTUM = 0.9
GELU_C = 0.7978845608028654
GELU_A = 0.044715
BF, F32 = jnp.bfloat16, jnp.float32

L, D, F, R = 12, 512, 2048, 512
FT = 256
TPL = F // FT
NC = L * TPL
NT = NC // 3
PR = 64
RING = 48
SLOTS, LAG, DEPTH = 4, 2, 13

CORE, DONE, OA, OB, OC, NTYPE = 0, 1, 2, 10, 18, 26
X, Y, ZU, ZD, GZU, GZD, GY, GX = range(8)
SLOT_PARTS = {}
for _base, _order in ((OA, "xyz"), (OB, "yzx"), (OC, "zxy")):
    for _n, _ax in zip((4, 2, 1), _order):
        for _ty in {"x": (X,), "y": (Y,), "z": (ZU, ZD)}[_ax]:
            SLOT_PARTS[_base + _ty] = _n


def gelu(a):
    return 0.5 * a * (1.0 + jnp.tanh(GELU_C * (a + GELU_A * (a * a * a))))


def gelu_both(a):
    sq = a * a
    th = jnp.tanh(GELU_C * (a + GELU_A * (sq * a)))
    half = 0.5 * (1.0 + th)
    slope = half + 0.5 * a * (1.0 - th * th) * (GELU_C * (1.0 + 3.0 * GELU_A * sq))
    return a * half, slope


def dot(a, b, da=1, db=0):
    return lax.dot_general(a, b, (((da,), (db,)), ((), ())), preferred_element_type=F32)


class Net:
    def __init__(self, part, out, slots, ssem, rsem, csem, ksem):
        self.part, self.out, self.slots = part, out, slots
        self.ssem, self.rsem, self.csem, self.ksem = ssem, rsem, csem, ksem
        pod, data = lax.axis_index("pod"), lax.axis_index("data")
        z, y, x, core = pod // 2, lax.rem(pod, 2), data // 2, lax.rem(data, 2)
        self.z, self.y, self.x, self.core = z, y, x, core
        dev = lambda z, y, x, core: (z * 2 + y, x * 2 + core)
        self.xn, self.yn, self.cn = dev(z, y, 1 - x, core), dev(z, 1 - y, x, core), dev(z, y, x, 1 - core)
        self.up, self.dn = dev(z + 1, y, x, core), dev(z - 1, y, x, core)
        self.has_up, self.has_dn = z < 3, z > 0
        self.end, self.d = (z == 0) | (z == 3), z // 3

    def neighbours(self):
        return ((self.xn, None), (self.yn, None), (self.cn, None), (self.up, self.has_up), (self.dn, self.has_dn))

    def each(self, fn):
        for i, (n, cond) in enumerate(self.neighbours()):
            go = functools.partial(fn, i, n)
            if cond is None:
                go()
            else:
                pl.when(cond)(go)

    def barrier(self):
        sem = pltpu.get_barrier_semaphore()
        self.each(lambda i, n: pl.semaphore_signal(sem, inc=1, device_id=n, device_id_type=MESH))
        pl.semaphore_wait(sem, 3 + jnp.where(self.has_up, 1, 0) + jnp.where(self.has_dn, 1, 0))

    def give_credit(self):
        file = (0, 1, 2, 4, 3)
        self.each(lambda i, n: pl.semaphore_signal(self.csem.at[file[i]], inc=1, device_id=n, device_id_type=MESH))

    def take_credit(self):
        self.each(lambda i, n: pl.semaphore_wait(self.csem.at[i], 1))

    def ok(self, t, cond=None):
        valid = (t >= 0) & (t < NT)
        return valid if cond is None else valid & cond

    def copy(self, ty, t, src, dst, to):
        s = lax.rem(t, SLOTS)
        return pltpu.make_async_remote_copy(src_ref=src, dst_ref=dst, send_sem=self.ssem.at[ty, s], recv_sem=self.rsem.at[ty, s],
                                            device_id=to, device_id_type=MESH)

    def slot(self, ty, t):
        return self.slots[ty].at[lax.rem(t, SLOTS)]

    def mine(self, c, first, n):
        return self.part.at[lax.rem(c, RING), pl.ds(first, n)]

    def full(self, c, first, n):
        return self.out.at[self.core, c, pl.ds(first, n)]

    def send(self, ty, t, cond, src, dst, to, like):
        pl.when(self.ok(t - 1, cond))(lambda: self.copy(ty, t - 1, like, like, to).wait_send())
        pl.when(self.ok(t, cond))(lambda: self.copy(ty, t, src, dst, to).start())

    def add(self, ty, t, cond, c, first, n, frm):
        def go():
            got = self.slot(ty, t)
            self.copy(ty, t, got, got, frm).wait_recv()
            row = lax.rem(c, RING)
            self.part[row, pl.ds(first, n)] = self.part[row, pl.ds(first, n)] + got[...]
        pl.when(self.ok(t, cond))(go)

    def pass_on(self, ty, t, cond, c, first, n, to):
        self.send(ty, t, cond, self.mine(c, first, n), self.slot(ty, t), to, self.mine(0, 0, n))

    def got(self, ty, t, cond, c, first, n, frm):
        ref = self.full(c, first, n)
        pl.when(self.ok(t, cond))(lambda: self.copy(ty, t, ref, ref, frm).wait_recv())

    def spread(self, ty, t, cond, c, first, n, to):
        self.send(ty, t, cond, self.full(c, first, n), self.full(c, first, n), to, self.mine(0, 0, n))

    def spread_own(self, ty, t, cond, c, first, n, to):
        self.send(ty, t, cond, self.mine(c, first, n), self.full(c, first, n), to, self.mine(0, 0, n))

    def keep(self, i, t, c, first):
        return pltpu.make_async_copy(self.mine(c, first, 1), self.full(c, first, 1), self.ksem.at[i])


def pump(net, s):
    z, y, x, d, end = net.z, net.y, net.x, net.d, net.end
    up, dn, xn, yn, cn = net.up, net.dn, net.xn, net.yn, net.cn
    a_u, a_d = 4 * x + 2 * y + 1, 4 * x + 2 * y
    b_u, b_d = 4 * y + 2, 4 * y
    c_u, c_d = 4, 0

    def z_reduce(base, k0, col, first_u, first_d, n):
        tu, td = s - (k0 + z), s - (k0 + 3 - z)
        cu, cd = 3 * tu + col, 3 * td + col
        net.add(base + ZU, tu, net.has_dn, cu, first_u, n, dn)
        net.pass_on(base + ZU, tu, net.has_up, cu, first_u, n, up)
        net.add(base + ZD, td, net.has_up, cd, first_d, n, up)
        net.pass_on(base + ZD, td, net.has_dn, cd, first_d, n, dn)

    def z_gather(base, k0, col, first_u, first_d, n, own):
        tu, td = s - (k0 + 3 - z), s - (k0 + z)
        cu, cd = 3 * tu + col, 3 * td + col
        mid = (z > 0) & (z < 3)
        net.got(base + GZU, tu, net.has_up, cu, first_u, n, up)
        if own:
            net.spread_own(base + GZU, tu, z == 3, cu, first_u, n, dn)
        net.spread(base + GZU, tu, mid if own else net.has_dn, cu, first_u, n, dn)
        net.got(base + GZD, td, net.has_dn, cd, first_d, n, dn)
        if own:
            net.spread_own(base + GZD, td, z == 0, cd, first_d, n, up)
        net.spread(base + GZD, td, mid if own else net.has_up, cd, first_d, n, up)

    t = s - 1
    net.pass_on(OA + X, t, None, 3 * t, 4 * (1 - x), 4, xn)
    net.pass_on(OB + Y, t, None, 3 * t + 1, 4 * (1 - y), 4, yn)
    z_reduce(OC, 1, 2, c_u, c_d, 4)
    t = s - 2
    net.add(OA + X, t, None, 3 * t, 4 * x, 4, xn)
    net.pass_on(OA + Y, t, None, 3 * t, 4 * x + 2 * (1 - y), 2, yn)
    net.add(OB + Y, t, None, 3 * t + 1, 4 * y, 4, yn)
    z_reduce(OB, 2, 1, b_u, b_d, 2)
    t = s - 3
    net.add(OA + Y, t, None, 3 * t, 4 * x + 2 * y, 2, yn)
    z_reduce(OA, 3, 0, a_u, a_d, 1)
    t = s - 4
    net.pass_on(OC + X, t, end, 3 * t + 2, 4 * d + 2 * (1 - x), 2, xn)
    t = s - 5
    net.add(OC + X, t, end, 3 * t + 2, 4 * d + 2 * x, 2, xn)
    net.pass_on(OC + Y, t, end, 3 * t + 2, 4 * d + 2 * x + 1 - y, 1, yn)
    net.pass_on(OB + X, t, end, 3 * t + 1, 4 * y + 2 * d + 1 - x, 1, xn)
    t = s - 6
    net.add(OC + Y, t, end, 3 * t + 2, 4 * d + 2 * x + y, 1, yn)
    net.add(OB + X, t, end, 3 * t + 1, 4 * y + 2 * d + x, 1, xn)
    own = [net.keep(0, t, 3 * t, 4 * x + 2 * y + d), net.keep(1, t, 3 * t + 1, 4 * y + 2 * d + x),
           net.keep(2, t, 3 * t + 2, 4 * d + 2 * x + y)]
    pl.when(net.ok(t, end))(lambda: [k.start() for k in own] and None)
    net.spread_own(OC + GY, t, end, 3 * t + 2, 4 * d + 2 * x + y, 1, yn)
    net.spread_own(OB + GX, t, end, 3 * t + 1, 4 * y + 2 * d + x, 1, xn)
    z_gather(OA, 6, 0, a_u, a_d, 1, True)
    pl.when(net.ok(t, end))(lambda: [k.wait() for k in own] and None)
    t = s - 7
    net.got(OC + GY, t, end, 3 * t + 2, 4 * d + 2 * x + 1 - y, 1, yn)
    net.spread(OC + GX, t, end, 3 * t + 2, 4 * d + 2 * x, 2, xn)
    net.got(OB + GX, t, end, 3 * t + 1, 4 * y + 2 * d + 1 - x, 1, xn)
    z_gather(OB, 7, 1, b_u, b_d, 2, False)
    t = s - 8
    net.got(OC + GX, t, end, 3 * t + 2, 4 * d + 2 * (1 - x), 2, xn)
    z_gather(OC, 8, 2, c_u, c_d, 4, False)
    t = s - 9
    net.spread(OA + GY, t, None, 3 * t, 4 * x + 2 * y, 2, yn)
    t = s - 10
    net.spread(OB + GY, t, None, 3 * t + 1, 4 * y, 4, yn)
    net.got(OA + GY, t, None, 3 * t, 4 * x + 2 * (1 - y), 2, yn)
    net.spread(OA + GX, t, None, 3 * t, 4 * x, 4, xn)
    t = s - 11
    net.got(OB + GY, t, None, 3 * t + 1, 4 * (1 - y), 4, yn)
    net.got(OA + GX, t, None, 3 * t, 4 * (1 - x), 4, xn)
    three = net.out.at[net.core, pl.ds(3 * t, 3)]
    net.send(DONE, t, None, three, three, cn, net.part.at[pl.ds(0, 3)])
    t = s - 12
    other = net.out.at[1 - net.core, pl.ds(3 * t, 3)]
    pl.when(net.ok(t))(lambda: net.copy(DONE, t, other, other, cn).wait_recv())


def exchange_kernel(scale, x_ref, y_ref, w1_ref, w2_ref, out_ref, h_ref, low_ref, saved_ref, w1_st, w2_st, gbuf, cslot, part,
                    wsem, ssem, rsem, csem, ksem, *slots):
    net = Net(part, out_ref, dict(zip(SLOT_PARTS, slots)), ssem, rsem, csem, ksem)
    core = net.core

    def weights(l):
        b = lax.rem(l, 2)
        return (pltpu.make_async_copy(w1_ref.at[l], w1_st.at[b], wsem.at[0, b]),
                pltpu.make_async_copy(w2_ref.at[l], w2_st.at[b], wsem.at[1, b]))

    def load(l):
        for c in weights(l):
            c.start()

    def loaded(l):
        for c in weights(l):
            c.wait()

    load(0)
    net.barrier()
    h_ref[...] = x_ref[...].astype(F32)

    @pl.loop(0, L)
    def _(l):
        pl.when(l < L - 1)(lambda: load(l + 1))
        loaded(l)
        b = lax.rem(l, 2)
        h_low = h_ref[...].astype(BF)
        saved_ref[l] = h_low
        tile = 512
        total = h_ref[...]
        for j in range(F // tile):
            w1 = w1_st[b, :, j * tile:(j + 1) * tile].astype(BF)
            act = gelu(dot(h_low, w1)).astype(BF)
            total = total + dot(act, w2_st[b, j * tile:(j + 1) * tile, :].astype(BF))
        h_ref[...] = total

    h_ref[...] = (h_ref[...] - y_ref[...].astype(F32)) * scale

    def backward(t, i):
        c = 3 * t + i
        l, j = L - 1 - c // TPL, lax.rem(c, TPL)
        b, col = lax.rem(l, 2), pl.multiple_of(j * FT, FT)

        @pl.when(j == 0)
        def _():
            pl.when(l < L - 2)(lambda: loaded(l))
            pl.when((l < L - 1) & (l > 0))(lambda: load(l - 1))
            low_ref[...] = h_ref[...].astype(BF)

        h_low, g_low = saved_ref[l], low_ref[...]
        w1 = w1_st[b, :, pl.ds(col, FT)].astype(BF)
        w2 = w2_st[b, pl.ds(col, FT), :].astype(BF)
        act, slope = gelu_both(dot(h_low, w1))
        q = (slope * dot(g_low, w2, 1, 1)).astype(BF)
        g2 = dot(act.astype(BF), g_low, 0, 0).astype(BF)
        g1 = dot(h_low, q, 0, 0).astype(BF)
        k = lax.rem(t, 2)
        gbuf[k, 0, i] = g1.reshape(8, PR, FT)
        gbuf[k, 1, i, 0:4] = g2[:, :FT].reshape(4, PR, FT)
        gbuf[k, 1, i, 4:8] = g2[:, FT:].reshape(4, PR, FT)
        h_ref[...] = h_ref[...] + dot(q, w1, 1, 1)

    def core_copy(t):
        return net.copy(CORE, t, gbuf.at[lax.rem(t, 2), 1 - core], net_slot(t), net.cn)

    def net_slot(t):
        return cslot.at[lax.rem(t, SLOTS)]

    def core_add(t):
        core_copy(t).wait_send()
        net.copy(CORE, t, net_slot(t), net_slot(t), net.cn).wait_recv()
        for i in range(3):
            part[lax.rem(3 * t + i, RING)] = gbuf[lax.rem(t, 2), core, i] + cslot[lax.rem(t, SLOTS), i]

    @pl.loop(0, NT + DEPTH)
    def _(s):
        pl.when(s >= LAG)(net.take_credit)
        pl.when(net.ok(s - 1))(lambda: core_add(s - 1))
        pump(net, s)

        @pl.when(net.ok(s))
        def _():
            @pl.loop(0, 3)
            def _(i):
                backward(s, i)
            core_copy(s).start()
        net.give_credit()

    for _ in range(LAG):
        net.take_credit()


def exchange(x_now, y_now, w_first, w_second, scale):
    vm = pl.BlockSpec(memory_space=pltpu.VMEM)
    hbm = pl.BlockSpec(memory_space=pl.ANY)
    return pl.pallas_call(
        functools.partial(exchange_kernel, scale),
        out_shape=jax.ShapeDtypeStruct((2, NC, 8, PR, FT), BF),
        in_specs=[vm, vm, hbm, hbm],
        out_specs=hbm,
        scratch_shapes=[
            pltpu.VMEM((R, D), F32), pltpu.VMEM((R, D), BF), pltpu.VMEM((L, R, D), BF),
            pltpu.VMEM((2, D, F), F32), pltpu.VMEM((2, F, D), F32),
            pltpu.VMEM((2, 2, 3, 8, PR, FT), BF), pltpu.VMEM((SLOTS, 3, 8, PR, FT), BF), pltpu.VMEM((RING, 8, PR, FT), BF),
            pltpu.SemaphoreType.DMA((2, 2)), pltpu.SemaphoreType.DMA((NTYPE, SLOTS)), pltpu.SemaphoreType.DMA((NTYPE, SLOTS)),
            pltpu.SemaphoreType.REGULAR((5,)), pltpu.SemaphoreType.DMA((3,)),
        ] + [pltpu.VMEM((SLOTS, n, PR, FT), BF) for n in SLOT_PARTS.values()],
        compiler_params=pltpu.CompilerParams(collective_id=0, has_side_effects=True, vmem_limit_bytes=63 * 2**20),
        name="exchange",
    )(x_now, y_now, w_first, w_second)


UT = 512


def update_kernel(rate, x_ref, g_ref, w1_ref, w2_ref, m1_ref, m2_ref, w1o, w2o, m1o, m2o, h_out, h_ref, low_ref):
    l, j = pl.program_id(0), pl.program_id(1)

    @pl.when((l == 0) & (j == 0))
    def _():
        h_ref[...] = x_ref[...].astype(F32)

    @pl.when(j == 0)
    def _():
        low_ref[...] = h_ref[...].astype(BF)

    n = UT // FT
    for k in range(n):
        cols = slice(k * FT, (k + 1) * FT)
        m = MOMENTUM * m1_ref[0, :, cols] + g_ref[0, k].reshape(D, FT).astype(F32)
        m1o[0, :, cols] = m
        w1o[0, :, cols] = w1_ref[0, :, cols] - rate * m
        for half in range(2):
            where = (0, slice(k * FT, (k + 1) * FT), slice(half * FT, (half + 1) * FT))
            m = MOMENTUM * m2_ref[where] + g_ref[1, k, 4 * half:4 * half + 4].reshape(FT, FT).astype(F32)
            m2o[where] = m
            w2o[where] = w2_ref[where] - rate * m
    act = gelu(dot(low_ref[...], w1o[0].astype(BF))).astype(BF)
    h_ref[...] = h_ref[...] + dot(act, w2o[0].astype(BF))

    @pl.when((l == L - 1) & (j == F // UT - 1))
    def _():
        h_out[...] = h_ref[...]


def update(x_next, grads, w_first, w_second, m_first, m_second, rate):
    tiles = F // UT
    first = pl.BlockSpec((1, D, UT), lambda l, j: (l, 0, j))
    second = pl.BlockSpec((1, UT, D), lambda l, j: (l, j, 0))
    whole = pl.BlockSpec((R, D), lambda l, j: (0, 0))
    chunks = pl.BlockSpec((2, UT // FT, 8, PR, FT), lambda l, j: (0, (L - 1 - l) * tiles + j, 0, 0, 0))
    return pl.pallas_call(
        functools.partial(update_kernel, rate),
        grid=(L, tiles),
        in_specs=[whole, chunks, first, second, first, second],
        out_specs=[first, second, first, second, whole],
        out_shape=[jax.ShapeDtypeStruct((L, D, F), F32), jax.ShapeDtypeStruct((L, F, D), F32)] * 2
        + [jax.ShapeDtypeStruct((R, D), F32)],
        scratch_shapes=[pltpu.VMEM((R, D), F32), pltpu.VMEM((R, D), BF)],
        compiler_params=pltpu.CompilerParams(vmem_limit_bytes=48 * 2**20, dimension_semantics=("arbitrary", "arbitrary")),
        cost_estimate=pl.CostEstimate(flops=4 * L * R * D * F, bytes_accessed=18 * 2 * L * D * F, transcendentals=L * R * F),
        name="update",
    )(x_next, grads, w_first, w_second, m_first, m_second)


def solution(mesh):
    rows_spec = P(("pod", "data"), None)
    full_spec = P()
    devices = mesh.shape["pod"] * mesh.shape["data"]

    def train_step(w_first, w_second, m_first, m_second, x_now, y_now, x_next, y_next):
        scale = 1.0 / (x_now.shape[0] * devices * D)
        grads = exchange(x_now, y_now, w_first, w_second, scale)
        w1, w2, m1, m2, hidden = update(x_next, grads, w_first, w_second, m_first, m_second, LEARN_BASE / L)
        resid = hidden - y_next.astype(F32)
        loss = jnp.sum(resid * resid, axis=-1) / (2 * D)
        return w1, w2, m1, m2, loss, hidden

    return jax.shard_map(train_step, mesh=mesh, in_specs=(full_spec,) * 4 + (rows_spec,) * 4,
                         out_specs=(full_spec,) * 4 + (P(("pod", "data")), rows_spec), check_vma=False)
```

```python
import functools

import jax
import jax.numpy as jnp
from jax import lax
from jax.experimental import pallas as pl
from jax.experimental.pallas import tpu as pltpu
from jax.sharding import PartitionSpec as P

MESH = pl.DeviceIdType.MESH
LEARN_BASE = 0.25
MOMENTUM = 0.9
GELU_C = 0.7978845608028654
GELU_A = 0.044715
BF, F32 = jnp.bfloat16, jnp.float32

L, D, F, R = 12, 512, 2048, 512
FT = 256
TPL = F // FT
NC = L * TPL
NT = NC // 3
LN = 128
TR = 3 * D * FT // LN
RING = 12
SLOTS, LAG, DEPTH = 4, 2, 15

CORE, DONE, OA, OB, OC, NTYPE = 0, 1, 2, 10, 20, 30
X, Y, ZU, ZD, GZU, GZD, GY, GX, W, GW = range(10)
FIRST_ROW = {OA: 0, OB: 1280, OC: 2176}
PART_ROWS = {OA: 160, OB: 112, OC: 112}
SLOT_ROWS = {}
for _base, _order in ((OA, "xyz"), (OB, "yzx"), (OC, "zxy")):
    for _n, _ax in zip((4, 2, 1), _order):
        for _ty in {"x": (X,), "y": (Y,), "z": (ZU, ZD) if _base == OA else (ZU, ZD, W)}[_ax]:
            SLOT_ROWS[_base + _ty] = _n * PART_ROWS[_base]


def gelu(a):
    return 0.5 * a * (1.0 + jnp.tanh(GELU_C * (a + GELU_A * (a * a * a))))


def gelu_both(a):
    sq = a * a
    th = jnp.tanh(GELU_C * (a + GELU_A * (sq * a)))
    half = 0.5 * (1.0 + th)
    slope = half + 0.5 * a * (1.0 - th * th) * (GELU_C * (1.0 + 3.0 * GELU_A * sq))
    return a * half, slope


def dot(a, b, da=1, db=0):
    return lax.dot_general(a, b, (((da,), (db,)), ((), ())), preferred_element_type=F32)


class Net:
    def __init__(self, part, out, slots, ssem, rsem, csem, ksem):
        self.part, self.out, self.slots = part, out, slots
        self.ssem, self.rsem, self.csem, self.ksem = ssem, rsem, csem, ksem
        pod, data = lax.axis_index("pod"), lax.axis_index("data")
        z, y, x, core = pod // 2, lax.rem(pod, 2), data // 2, lax.rem(data, 2)
        self.z, self.y, self.x, self.core = z, y, x, core
        self.at = lambda z: (z * 2 + y, x * 2 + core)
        self.xn, self.yn, self.cn = (pod, 2 * (1 - x) + core), (z * 2 + 1 - y, data), (pod, 2 * x + 1 - core)
        self.up, self.dn = self.at(z + 1), self.at(z - 1)
        self.cross = self.at(jnp.where(lax.rem(z, 2) == 0, z + 1, z - 1))
        self.d = z // 2
        self.sent = []

    def neighbours(self):
        return ((self.xn, None), (self.yn, None), (self.cn, None), (self.up, self.z < 3), (self.dn, self.z > 0))

    def each(self, fn):
        for i, (n, cond) in enumerate(self.neighbours()):
            go = functools.partial(fn, i, n)
            if cond is None:
                go()
            else:
                pl.when(cond)(go)

    def greet(self):
        sem = pltpu.get_barrier_semaphore()
        self.each(lambda i, n: pl.semaphore_signal(sem, inc=1, device_id=n, device_id_type=MESH))

    def greeted(self):
        pl.semaphore_wait(pltpu.get_barrier_semaphore(), 3 + jnp.where(self.z < 3, 1, 0) + jnp.where(self.z > 0, 1, 0))

    def give_credit(self):
        file = (0, 1, 2, 4, 3)
        self.each(lambda i, n: pl.semaphore_signal(self.csem.at[file[i]], inc=1, device_id=n, device_id_type=MESH))

    def take_credit(self):
        self.each(lambda i, n: pl.semaphore_wait(self.csem.at[i], 1))

    def copy(self, ty, t, src, dst, to):
        s = lax.rem(t, SLOTS)
        return pltpu.make_async_remote_copy(src_ref=src, dst_ref=dst, send_sem=self.ssem.at[ty, s], recv_sem=self.rsem.at[ty, s],
                                            device_id=to, device_id_type=MESH)

    def slot(self, ty, t):
        return self.slots[ty].at[lax.rem(t, SLOTS)]

    def rows(self, base, first, n):
        return pl.ds(pl.multiple_of(FIRST_ROW[base] + first * PART_ROWS[base], 16), n * PART_ROWS[base])

    def mine(self, base, t, first, n):
        return self.part.at[lax.rem(t, RING), self.rows(base, first, n)]

    def full(self, base, t, first, n):
        return self.out.at[self.core, t, self.rows(base, first, n)]

    def send(self, ty, t, src, dst, to, like, cond=None):
        pl.when(t >= SLOTS)(lambda: self.copy(ty, t - SLOTS, like(), like(), to).wait_send())
        self.copy(ty, t, src, dst, to).start()
        self.sent.append((ty, like, to, cond))

    def all_sent(self):
        for ty, like, to, cond in self.sent:
            for t in (NT - 4, NT - 3):
                def go(t=t):
                    for u in (t, t + 2):
                        self.copy(ty, u, like(), like(), to).wait_send()
                if cond is None:
                    go()
                else:
                    pl.when(cond(t))(go)

    def add(self, base, kind, t, first, n, frm):
        got = self.slot(base + kind, t)
        self.copy(base + kind, t, got, got, frm).wait_recv()
        row, rows = lax.rem(t, RING), self.rows(base, first, n)
        self.part[row, rows] = self.part[row, rows] + got[...]

    def pass_on(self, base, kind, t, first, n, to, cond=None):
        self.send(base + kind, t, self.mine(base, t, first, n), self.slot(base + kind, t), to, lambda: self.mine(base, 0, 0, n), cond)

    def got(self, base, kind, t, first, n, frm):
        ref = self.full(base, t, first, n)
        self.copy(base + kind, t, ref, ref, frm).wait_recv()

    def spread(self, base, kind, t, first, n, to, cond=None, own=False):
        full = self.full(base, t, first, n)
        self.send(base + kind, t, self.mine(base, t, first, n) if own else full, full, to, lambda: self.mine(base, 0, 0, n), cond)

    def keep(self, i, base, t, first):
        return pltpu.make_async_copy(self.mine(base, t, first, 1), self.full(base, t, first, 1), self.ksem.at[i])


class Momentum:
    def __init__(self, out, old, new, tiles, grads, sems):
        self.out, self.old, self.new, self.tiles, self.grads, self.sems = out, old, new, tiles, grads, sems

    def copies(self, t, back):
        k = lax.rem(t, 2)
        for i in range(3):
            c = 3 * t + i
            l, cols = L - 1 - c // TPL, pl.ds(pl.multiple_of(lax.rem(c, TPL) * FT, FT), FT)
            for w, where in enumerate(((l, slice(None), cols), (l, cols))):
                tile, sem = self.tiles[w].at[k, i], self.sems.at[int(back), w, k, i]
                if back:
                    yield pltpu.make_async_copy(tile, self.new[w].at[where], sem)
                else:
                    yield pltpu.make_async_copy(self.old[w].at[where], tile, sem)
        if not back:
            yield pltpu.make_async_copy(self.out.at[:, t], self.grads.at[k], self.sems.at[2, 0, k, 0])

    def load(self, t):
        for c in self.copies(t, False):
            c.start()

    def update(self, t):
        for c in self.copies(t, False):
            c.wait()
        k = lax.rem(t, 2)
        for i in range(3):
            row = i * (TR // 3)
            for w, (tile, n) in enumerate(zip(self.tiles, (D, FT))):
                for q in range(TR // 3 // n):
                    cols = slice(q * LN, (q + 1) * LN)
                    tile[k, i, :, cols] = MOMENTUM * tile[k, i, :, cols] + self.grads[k, w, row + q * n:row + (q + 1) * n].astype(F32)
        for c in self.copies(t, True):
            c.start()

    def stored(self, t):
        for c in self.copies(t, True):
            c.wait()


def valid(t):
    return (t >= 0) & (t < NT)


def pump(net, s, compute, momentum):
    z, y, x, d = net.z, net.y, net.x, net.d
    up, dn, xn, yn, cn, cross = net.up, net.dn, net.xn, net.yn, net.cn, net.cross
    side = lambda: (z == 0) | (z == 3)

    def mode(base, t):
        if base == OA:
            return 0
        return t % 2 if isinstance(t, int) else lax.rem(t, 2)

    def owner(base):
        return lambda t: z == 3 * d + mode(base, t) * (1 - 2 * d)

    def if_(t, cond, *acts):
        @pl.when(cond(t))
        def _():
            for act in acts:
                act()

    def stage(k, fn):
        t = s - k
        pl.when(valid(t))(lambda: fn(t))

    def add(*a):
        return lambda: net.add(*a)

    def got(*a):
        return lambda: net.got(*a)

    def pass_on(*a):
        return lambda: net.pass_on(*a)

    def spread(*a, **k):
        return lambda: net.spread(*a, **k)

    def z_reduce(base, k0, first_u, first_d, n):
        def climb(t):
            to_up = lambda t: z < 3 - mode(base, t)
            if_(t, lambda t: (z > 0) & (z <= 3 - mode(base, t)), add(base, ZU, t, first_u, n, dn))
            if_(t, to_up, pass_on(base, ZU, t, first_u, n, up, to_up))

        def sink(t):
            to_dn = lambda t: z > mode(base, t)
            if_(t, lambda t: (z < 3) & (z >= mode(base, t)), add(base, ZD, t, first_d, n, up))
            if_(t, to_dn, pass_on(base, ZD, t, first_d, n, dn, to_dn))

        stage(k0 + z, climb)
        stage(k0 + 3 - z, sink)
        if base != OA:
            f = jnp.where(z >= 2, first_u, first_d)
            give = lambda t: side() & (mode(base, t) == 1)
            stage(k0, lambda t: if_(t, give, pass_on(base, W, t, f, n, cross, give)))
            stage(k0 + 1, lambda t: if_(t, lambda t: ~side() & (mode(base, t) == 1), add(base, W, t, f, n, cross)))

    def z_gather(base, k0, first_u, first_d, n):
        own = base == OA

        def sink(t):
            to_dn = lambda t: (z > 0) & (z <= (2 if own else 3 - mode(base, t)))
            if_(t, lambda t: z < 3 - mode(base, t), got(base, GZU, t, first_u, n, up))
            if own:
                top = lambda t: z == 3
                if_(t, top, spread(base, GZU, t, first_u, n, dn, top, own=True))
            if_(t, to_dn, spread(base, GZU, t, first_u, n, dn, to_dn))

        def climb(t):
            to_up = lambda t: (z < 3) & (z >= (1 if own else mode(base, t)))
            if_(t, lambda t: z > mode(base, t), got(base, GZD, t, first_d, n, dn))
            if own:
                bottom = lambda t: z == 0
                if_(t, bottom, spread(base, GZD, t, first_d, n, up, bottom, own=True))
            if_(t, to_up, spread(base, GZD, t, first_d, n, up, to_up))

        stage(k0 + 3 - z, sink)
        stage(k0 + z, climb)
        if not own:
            f = jnp.where(z >= 2, first_u, first_d)
            give = lambda t: ~side() & (mode(base, t) == 1)
            stage(k0 + 1, lambda t: if_(t, give, spread(base, GW, t, f, n, cross, give)))
            stage(k0 + 2, lambda t: if_(t, lambda t: side() & (mode(base, t) == 1), got(base, GW, t, f, n, cross)))

    own_a, own_b, own_c = 4 * x + 2 * y + d, 4 * y + 2 * d + x, 4 * d + 2 * x + y

    def kept(t):
        for i, (base, first) in enumerate(((OA, own_a), (OB, own_b), (OC, own_c))):
            if_(t, owner(base), net.keep(i, base, t, first).wait)

    def k1(t):
        net.pass_on(OA, X, t, 4 * (1 - x), 4, xn)
        net.pass_on(OB, Y, t, 4 * (1 - y), 4, yn)

    def k2(t):
        net.add(OA, X, t, 4 * x, 4, xn)
        net.pass_on(OA, Y, t, 4 * x + 2 * (1 - y), 2, yn)
        net.add(OB, Y, t, 4 * y, 4, yn)

    def k4(t):
        if_(t, owner(OC), pass_on(OC, X, t, 4 * d + 2 * (1 - x), 2, xn, owner(OC)))

    def k5(t):
        if_(t, owner(OC), add(OC, X, t, 4 * d + 2 * x, 2, xn),
            pass_on(OC, Y, t, 4 * d + 2 * x + 1 - y, 1, yn, owner(OC)))
        if_(t, owner(OB), pass_on(OB, X, t, 4 * y + 2 * d + 1 - x, 1, xn, owner(OB)))

    def k6(t):
        if_(t, owner(OC), add(OC, Y, t, own_c, 1, yn), net.keep(2, OC, t, own_c).start,
            spread(OC, GY, t, own_c, 1, yn, owner(OC), own=True))
        if_(t, owner(OB), add(OB, X, t, own_b, 1, xn), net.keep(1, OB, t, own_b).start,
            spread(OB, GX, t, own_b, 1, xn, owner(OB), own=True))

    def k7(t):
        if_(t, owner(OC), got(OC, GY, t, 4 * d + 2 * x + 1 - y, 1, yn), spread(OC, GX, t, 4 * d + 2 * x, 2, xn, owner(OC)))
        if_(t, owner(OB), got(OB, GX, t, 4 * y + 2 * d + 1 - x, 1, xn))

    def k10(t):
        net.spread(OB, GY, t, 4 * y, 4, yn)
        net.got(OA, GY, t, 4 * x + 2 * (1 - y), 2, yn)
        net.spread(OA, GX, t, 4 * x, 4, xn)

    def k11(t):
        net.got(OB, GY, t, 4 * (1 - y), 4, yn)
        net.got(OA, GX, t, 4 * (1 - x), 4, xn)
        triple = net.out.at[net.core, t]
        net.send(DONE, t, triple, triple, cn, lambda: net.part.at[0])

    def k12(t):
        other = net.out.at[1 - net.core, t]
        net.copy(DONE, t, other, other, cn).wait_recv()

    stage(7, kept)
    stage(1, k1)
    z_reduce(OC, 1, 4, 0, 4)
    compute(0)
    stage(2, k2)
    z_reduce(OB, 2, 4 * y + 2, 4 * y, 2)
    stage(3, lambda t: net.add(OA, Y, t, 4 * x + 2 * y, 2, yn))
    z_reduce(OA, 3, 4 * x + 2 * y + 1, 4 * x + 2 * y, 1)
    stage(4, k4)
    stage(5, k5)
    compute(1)
    stage(6, k6)
    stage(6, lambda t: if_(t, owner(OA), net.keep(0, OA, t, own_a).start))
    z_gather(OA, 6, 4 * x + 2 * y + 1, 4 * x + 2 * y, 1)
    stage(7, k7)
    z_gather(OB, 7, 4 * y + 2, 4 * y, 2)
    stage(8, lambda t: if_(t, owner(OC), got(OC, GX, t, 4 * d + 2 * (1 - x), 2, xn)))
    z_gather(OC, 8, 4, 0, 4)
    compute(2)
    stage(9, lambda t: net.spread(OA, GY, t, 4 * x + 2 * y, 2, yn))
    stage(10, k10)
    stage(11, k11)
    stage(14, momentum.stored)
    stage(12, k12)
    stage(12, momentum.load)
    stage(13, momentum.update)


def exchange_kernel(scale, x_ref, y_ref, w1_ref, w2_ref, m1_ref, m2_ref, out_ref, m1_new, m2_new, h_ref, low_ref, turn_ref, saved_ref, w1_st, w2_st, gbuf, cslot, part,
                    tile1, tile2, grads, wsem, psem, msem, ssem, rsem, csem, ksem, *slots):
    net = Net(part, out_ref, dict(zip(SLOT_ROWS, slots)), ssem, rsem, csem, ksem)
    core = net.core
    momentum = Momentum(out_ref, (m1_ref, m2_ref), (m1_new, m2_new), (tile1, tile2), grads, msem)

    half = F // 2

    def weights(i):
        b, cols = lax.rem(i, 4), pl.ds(pl.multiple_of(lax.rem(i, 2) * half, half), half)
        return (pltpu.make_async_copy(w1_ref.at[i // 2, :, cols], w1_st.at[b], wsem.at[0, b]),
                pltpu.make_async_copy(w2_ref.at[i // 2, cols, :], w2_st.at[b], wsem.at[1, b]))

    def load(i):
        for c in weights(i):
            c.start()

    def loaded(i):
        for c in weights(i):
            c.wait()

    net.greet()
    for i in range(3):
        load(i)
    h_ref[...] = x_ref[...].astype(F32)

    @pl.loop(0, 2 * L)
    def _(i):
        pl.when(i < 2 * L - 3)(lambda: load(i + 3))
        l, b = i // 2, lax.rem(i, 4)

        @pl.when(lax.rem(i, 2) == 0)
        def _():
            saved_ref[l] = h_ref[...].astype(BF)
        loaded(i)
        act = gelu(dot(saved_ref[l], w1_st[b].astype(BF))).astype(BF)
        h_ref[...] = h_ref[...] + dot(act, w2_st[b].astype(BF))

    h_ref[...] = (h_ref[...] - y_ref[...].astype(F32)) * scale

    def backward(t, i):
        c = 3 * t + i
        l, j = L - 1 - c // TPL, lax.rem(c, TPL)
        i0 = 2 * l
        b, col = lax.rem(i0 + j // (TPL // 2), 4), pl.multiple_of(lax.rem(j, TPL // 2) * FT, FT)

        def piece(l):
            i = 2 * l + j // (TPL // 2)
            b, to = lax.rem(i, 4), pl.ds(col, FT)
            frm = pl.ds(pl.multiple_of(j * FT, FT), FT)
            return (pltpu.make_async_copy(w1_ref.at[l, :, frm], w1_st.at[b, :, to], psem.at[0, lax.rem(l, 2), j]),
                    pltpu.make_async_copy(w2_ref.at[l, frm, :], w2_st.at[b, to, :], psem.at[1, lax.rem(l, 2), j]))

        @pl.when((l < L - 1) & (l > 0))
        def _():
            for p in piece(l - 1):
                p.start()

        @pl.when(l < L - 2)
        def _():
            for p in piece(l):
                p.wait()

        @pl.when(j == 0)
        def _():
            low_ref[...] = h_ref[...].astype(BF)
            turn_ref[...] = saved_ref[l].T

        h_low, g_low = saved_ref[l], low_ref[...]
        w1 = w1_st[b, :, pl.ds(col, FT)].astype(BF)
        w2 = w2_st[b, pl.ds(col, FT), :].astype(BF)
        act, slope = gelu_both(dot(h_low, w1))
        q = (slope * dot(g_low, w2, 1, 1)).astype(BF)
        g2 = dot(act.astype(BF), g_low, 0, 0).astype(BF)
        g1 = dot(turn_ref[...], q).astype(BF)
        k, row = lax.rem(t, 2), i * (TR // 3)
        for half in range(FT // LN):
            gbuf[k, 0, pl.ds(row + half * D, D)] = g1[:, half * LN:(half + 1) * LN]
        for q4 in range(D // LN):
            gbuf[k, 1, pl.ds(row + q4 * FT, FT)] = g2[:, q4 * LN:(q4 + 1) * LN]
        h_ref[...] = h_ref[...] + dot(q, w1, 1, 1)

    def core_copy(t):
        return net.copy(CORE, t, gbuf.at[lax.rem(t, 2), 1 - core], net_slot(t), net.cn)

    def net_slot(t):
        return cslot.at[lax.rem(t, SLOTS)]

    def core_add(t):
        core_copy(t).wait_send()
        net.copy(CORE, t, net_slot(t), net_slot(t), net.cn).wait_recv()
        part[lax.rem(t, RING)] = gbuf[lax.rem(t, 2), core] + cslot[lax.rem(t, SLOTS)]

    net.greeted()

    @pl.loop(0, NT + DEPTH)
    def _(s):
        pl.when(s >= LAG)(net.take_credit)
        pl.when(valid(s - 1))(lambda: core_add(s - 1))
        def compute(i):
            @pl.when(valid(s))
            def _():
                backward(s, i)
                if i == 2:
                    core_copy(s).start()

        pump(net, s, compute, momentum)
        net.give_credit()

    net.all_sent()
    for _ in range(LAG):
        net.take_credit()


def exchange(x_now, y_now, w_first, w_second, m_first, m_second, scale):
    vm = pl.BlockSpec(memory_space=pltpu.VMEM)
    hbm = pl.BlockSpec(memory_space=pl.ANY)
    return pl.pallas_call(
        functools.partial(exchange_kernel, scale),
        out_shape=[jax.ShapeDtypeStruct((2, NT, TR, LN), BF), jax.ShapeDtypeStruct((L, D, F), F32),
                   jax.ShapeDtypeStruct((L, F, D), F32)],
        in_specs=[vm, vm] + [hbm] * 4,
        out_specs=[hbm] * 3,
        scratch_shapes=[
            pltpu.VMEM((R, D), F32), pltpu.VMEM((R, D), BF), pltpu.VMEM((D, R), BF), pltpu.VMEM((L, R, D), BF),
            pltpu.VMEM((4, D, F // 2), F32), pltpu.VMEM((4, F // 2, D), F32),
            pltpu.VMEM((2, 2, TR, LN), BF), pltpu.VMEM((SLOTS, TR, LN), BF), pltpu.VMEM((RING, TR, LN), BF),
            pltpu.VMEM((2, 3, D, FT), F32), pltpu.VMEM((2, 3, FT, D), F32), pltpu.VMEM((2, 2, TR, LN), BF),
            pltpu.SemaphoreType.DMA((2, 4)), pltpu.SemaphoreType.DMA((2, 2, TPL)), pltpu.SemaphoreType.DMA((3, 2, 2, 3)), pltpu.SemaphoreType.DMA((NTYPE, SLOTS)), pltpu.SemaphoreType.DMA((NTYPE, SLOTS)),
            pltpu.SemaphoreType.REGULAR((5,)), pltpu.SemaphoreType.DMA((3,)),
        ] + [pltpu.VMEM((SLOTS, n, LN), BF) for n in SLOT_ROWS.values()],
        compiler_params=pltpu.CompilerParams(collective_id=0, has_side_effects=True, vmem_limit_bytes=63 * 2**20),
        name="exchange",
    )(x_now, y_now, w_first, w_second, m_first, m_second)


UT = 512
TILES = F // UT
BUFS, AHEAD = 8, 4


def update_kernel(rate, x_ref, w1_ref, w2_ref, m1_ref, m2_ref, w1o, w2o, m1o, m2o, h_ref, low_ref, w1, w2, m1, m2, isem, osem):
    olds, news, tiles = (w1_ref, w2_ref, m1_ref, m2_ref), (w1o, w2o, m1o, m2o), (w1, w2, m1, m2)

    def copy(a, i, back):
        l, cols = i // TILES, pl.ds(pl.multiple_of(lax.rem(i, TILES) * UT, UT), UT)
        where = (l, slice(None), cols) if a % 2 == 0 else (l, cols)
        k = lax.rem(i, BUFS)
        if back:
            return pltpu.make_async_copy(tiles[a].at[k], news[a].at[where], osem.at[a, k])
        return pltpu.make_async_copy(olds[a].at[where], tiles[a].at[k], isem.at[a, k])

    def load(i):
        for a in range(4):
            copy(a, i, False).start()

    def stored(i):
        for a in range(4):
            copy(a, i, True).wait()

    for i in range(AHEAD):
        load(i)
    h_ref[...] = x_ref[...].astype(F32)

    @pl.loop(0, L * TILES)
    def _(i):
        pl.when(i + AHEAD >= BUFS)(lambda: pl.when(i + AHEAD < L * TILES)(lambda: stored(i + AHEAD - BUFS)))
        pl.when(i + AHEAD < L * TILES)(lambda: load(i + AHEAD))

        @pl.when(lax.rem(i, TILES) == 0)
        def _():
            low_ref[...] = h_ref[...].astype(BF)

        for a in range(4):
            copy(a, i, False).wait()
        for a in (2, 3):
            copy(a, i, True).start()
        k = lax.rem(i, BUFS)
        first = w1[k] - rate * m1[k]
        w1[k] = first
        copy(0, i, True).start()
        act = gelu(dot(low_ref[...], first.astype(BF))).astype(BF)
        second = w2[k] - rate * m2[k]
        w2[k] = second
        copy(1, i, True).start()
        h_ref[...] = h_ref[...] + dot(act, second.astype(BF))

    @pl.loop(L * TILES - BUFS, L * TILES)
    def _(i):
        stored(i)


def update(x_next, w_first, w_second, m_first, m_second, rate):
    vm = pl.BlockSpec(memory_space=pltpu.VMEM)
    hbm = pl.BlockSpec(memory_space=pl.ANY)
    return pl.pallas_call(
        functools.partial(update_kernel, rate),
        in_specs=[vm] + [hbm] * 4,
        out_specs=[hbm] * 4 + [vm],
        out_shape=[jax.ShapeDtypeStruct((L, D, F), F32), jax.ShapeDtypeStruct((L, F, D), F32)] * 2
        + [jax.ShapeDtypeStruct((R, D), F32)],
        scratch_shapes=[pltpu.VMEM((R, D), BF)] + [pltpu.VMEM((BUFS, D, UT), F32), pltpu.VMEM((BUFS, UT, D), F32)] * 2
        + [pltpu.SemaphoreType.DMA((4, BUFS))] * 2,
        compiler_params=pltpu.CompilerParams(vmem_limit_bytes=60 * 2**20),
        cost_estimate=pl.CostEstimate(flops=4 * L * R * D * F, bytes_accessed=16 * 2 * L * D * F, transcendentals=L * R * F),
        name="update",
    )(x_next, w_first, w_second, m_first, m_second)


def solution(mesh):
    rows_spec = P(("pod", "data"), None)
    full_spec = P()
    devices = mesh.shape["pod"] * mesh.shape["data"]

    def train_step(w_first, w_second, m_first, m_second, x_now, y_now, x_next, y_next):
        scale = 1.0 / (x_now.shape[0] * devices * D)
        _, m_first, m_second = exchange(x_now, y_now, w_first, w_second, m_first, m_second, scale)
        w1, w2, m1, m2, hidden = update(x_next, w_first, w_second, m_first, m_second, LEARN_BASE / L)
        resid = hidden - y_next.astype(F32)
        loss = jnp.sum(resid * resid, axis=-1) / (2 * D)
        return w1, w2, m1, m2, loss, hidden

    return jax.shard_map(train_step, mesh=mesh, in_specs=(full_spec,) * 4 + (rows_spec,) * 4,
                         out_specs=(full_spec,) * 4 + (P(("pod", "data")), rows_spec), check_vma=False)
```

```python
import functools

import jax
import jax.numpy as jnp
from jax import lax
from jax.experimental import pallas as pl
from jax.experimental.pallas import tpu as pltpu
from jax.sharding import PartitionSpec as P

MESH = pl.DeviceIdType.MESH
LEARN_BASE = 0.25
MOMENTUM = 0.9
GELU_C = 0.7978845608028654
GELU_A = 0.044715
BF, F32 = jnp.bfloat16, jnp.float32

L, D, F, R = 12, 512, 2048, 512
FT = 256
TPL = F // FT
NC = L * TPL
NT = NC // 3
LN = 128
TR = 3 * D * FT // LN
RING = 12
SLOTS, LAG, DEPTH = 4, 2, 15

CORE, DONE, OA, OB, OC, NTYPE = 0, 1, 2, 10, 20, 30
X, Y, ZU, ZD, GZU, GZD, GY, GX, W, GW = range(10)
FIRST_ROW = {OA: 0, OB: 1280, OC: 2176}
PART_ROWS = {OA: 160, OB: 112, OC: 112}
SLOT_ROWS = {}
for _base, _order in ((OA, "xyz"), (OB, "yzx"), (OC, "zxy")):
    for _n, _ax in zip((4, 2, 1), _order):
        for _ty in {"x": (X,), "y": (Y,), "z": (ZU, ZD, W) if _base == OC else (ZU, ZD)}[_ax]:
            SLOT_ROWS[_base + _ty] = _n * PART_ROWS[_base]


def gelu(a):
    return 0.5 * a * (1.0 + jnp.tanh(GELU_C * (a + GELU_A * (a * a * a))))


def gelu_both(a):
    sq = a * a
    th = jnp.tanh(GELU_C * (a + GELU_A * (sq * a)))
    half = 0.5 * (1.0 + th)
    slope = half + 0.5 * a * (1.0 - th * th) * (GELU_C * (1.0 + 3.0 * GELU_A * sq))
    return a * half, slope


def dot(a, b, da=1, db=0):
    return lax.dot_general(a, b, (((da,), (db,)), ((), ())), preferred_element_type=F32)


class Net:
    def __init__(self, part, out, slots, ssem, rsem, csem, ksem):
        self.part, self.out, self.slots = part, out, slots
        self.ssem, self.rsem, self.csem, self.ksem = ssem, rsem, csem, ksem
        pod, data = lax.axis_index("pod"), lax.axis_index("data")
        z, y, x, core = pod // 2, lax.rem(pod, 2), data // 2, lax.rem(data, 2)
        self.z, self.y, self.x, self.core = z, y, x, core
        self.at = lambda z: (z * 2 + y, x * 2 + core)
        self.xn, self.yn, self.cn = (pod, 2 * (1 - x) + core), (z * 2 + 1 - y, data), (pod, 2 * x + 1 - core)
        self.up, self.dn = self.at(z + 1), self.at(z - 1)
        self.cross = self.at(jnp.where(lax.rem(z, 2) == 0, z + 1, z - 1))
        self.d = z // 2
        self.sent = []

    def neighbours(self):
        return ((self.xn, None), (self.yn, None), (self.cn, None), (self.up, self.z < 3), (self.dn, self.z > 0))

    def each(self, fn):
        for i, (n, cond) in enumerate(self.neighbours()):
            go = functools.partial(fn, i, n)
            if cond is None:
                go()
            else:
                pl.when(cond)(go)

    def greet(self):
        sem = pltpu.get_barrier_semaphore()
        self.each(lambda i, n: pl.semaphore_signal(sem, inc=1, device_id=n, device_id_type=MESH))

    def greeted(self):
        pl.semaphore_wait(pltpu.get_barrier_semaphore(), 3 + jnp.where(self.z < 3, 1, 0) + jnp.where(self.z > 0, 1, 0))

    def give_credit(self):
        file = (0, 1, 2, 4, 3)
        self.each(lambda i, n: pl.semaphore_signal(self.csem.at[file[i]], inc=1, device_id=n, device_id_type=MESH))

    def take_credit(self):
        self.each(lambda i, n: pl.semaphore_wait(self.csem.at[i], 1))

    def copy(self, ty, t, src, dst, to):
        s = lax.rem(t, SLOTS)
        return pltpu.make_async_remote_copy(src_ref=src, dst_ref=dst, send_sem=self.ssem.at[ty, s], recv_sem=self.rsem.at[ty, s],
                                            device_id=to, device_id_type=MESH)

    def slot(self, ty, t):
        return self.slots[ty].at[lax.rem(t, SLOTS)]

    def rows(self, base, first, n):
        return pl.ds(pl.multiple_of(FIRST_ROW[base] + first * PART_ROWS[base], 16), n * PART_ROWS[base])

    def mine(self, base, t, first, n):
        return self.part.at[lax.rem(t, RING), self.rows(base, first, n)]

    def full(self, base, t, first, n):
        return self.out.at[self.core, t, self.rows(base, first, n)]

    def send(self, ty, t, src, dst, to, like, cond=None):
        if cond is None:
            self.wait_old(ty, t, like, to)
        self.copy(ty, t, src, dst, to).start()
        self.sent.append((ty, like, to, cond))

    def wait_old(self, ty, t, like, to, cond=None):
        was = t >= SLOTS if cond is None else (t >= SLOTS) & cond(t - SLOTS)
        pl.when(was)(lambda: self.copy(ty, t - SLOTS, like(), like(), to).wait_send())

    def all_sent(self):
        for ty, like, to, cond in self.sent:
            for t in range(NT - SLOTS, NT):
                def go(t=t):
                    self.copy(ty, t, like(), like(), to).wait_send()
                if cond is None:
                    go()
                else:
                    pl.when(cond(t))(go)

    def add(self, base, kind, t, first, n, frm):
        got = self.slot(base + kind, t)
        self.copy(base + kind, t, got, got, frm).wait_recv()
        row, rows = lax.rem(t, RING), self.rows(base, first, n)
        self.part[row, rows] = self.part[row, rows] + got[...]

    def pass_on(self, base, kind, t, first, n, to, cond=None):
        self.send(base + kind, t, self.mine(base, t, first, n), self.slot(base + kind, t), to, lambda: self.mine(base, 0, 0, n), cond)

    def got(self, base, kind, t, first, n, frm):
        ref = self.full(base, t, first, n)
        self.copy(base + kind, t, ref, ref, frm).wait_recv()

    def spread(self, base, kind, t, first, n, to, cond=None, own=False):
        full = self.full(base, t, first, n)
        self.send(base + kind, t, self.mine(base, t, first, n) if own else full, full, to, lambda: self.mine(base, 0, 0, n), cond)

    def keep(self, i, base, t, first):
        return pltpu.make_async_copy(self.mine(base, t, first, 1), self.full(base, t, first, 1), self.ksem.at[i])


class Momentum:
    def __init__(self, out, old, new, tiles, grads, sems):
        self.out, self.old, self.new, self.tiles, self.grads, self.sems = out, old, new, tiles, grads, sems

    def copies(self, t, back):
        k = lax.rem(t, 2)
        for i in range(3):
            c = 3 * t + i
            l, cols = L - 1 - c // TPL, pl.ds(pl.multiple_of(lax.rem(c, TPL) * FT, FT), FT)
            for w, where in enumerate(((l, slice(None), cols), (l, cols))):
                tile, sem = self.tiles[w].at[k, i], self.sems.at[int(back), w, k, i]
                if back:
                    yield pltpu.make_async_copy(tile, self.new[w].at[where], sem)
                else:
                    yield pltpu.make_async_copy(self.old[w].at[where], tile, sem)
        if not back:
            yield pltpu.make_async_copy(self.out.at[:, t], self.grads.at[k], self.sems.at[2, 0, k, 0])

    def load(self, t):
        for c in self.copies(t, False):
            c.start()

    def update(self, t):
        for c in self.copies(t, False):
            c.wait()
        k = lax.rem(t, 2)
        for i in range(3):
            row = i * (TR // 3)
            for w, (tile, n) in enumerate(zip(self.tiles, (D, FT))):
                for q in range(TR // 3 // n):
                    cols = slice(q * LN, (q + 1) * LN)
                    tile[k, i, :, cols] = MOMENTUM * tile[k, i, :, cols] + self.grads[k, w, row + q * n:row + (q + 1) * n].astype(F32)
        for c in self.copies(t, True):
            c.start()

    def stored(self, t):
        for c in self.copies(t, True):
            c.wait()


def valid(t):
    return (t >= 0) & (t < NT)


def pump(net, s, compute, momentum):
    z, y, x, d = net.z, net.y, net.x, net.d
    up, dn, xn, yn, cn, cross = net.up, net.dn, net.xn, net.yn, net.cn, net.cross
    side = lambda: (z == 0) | (z == 3)

    def mode(base, t):
        if base != OC:
            return 0
        return t % 7 % 2 if isinstance(t, int) else lax.rem(lax.rem(t + 14, 7), 2)

    def owner(base):
        return lambda t: z == 3 * d + mode(base, t) * (1 - 2 * d)

    def if_(t, cond, *acts):
        for act in acts:
            if hasattr(act, "before"):
                act.before()

        @pl.when(cond(t))
        def _():
            for act in acts:
                act()

    def stage(k, fn):
        t = s - k
        pl.when(valid(t))(lambda: fn(t))

    def add(*a):
        return lambda: net.add(*a)

    def got(*a):
        return lambda: net.got(*a)

    def sender(fn, base, kind, t, first, n, to, cond, **k):
        def act():
            fn(base, kind, t, first, n, to, cond, **k)
        act.before = lambda: net.wait_old(base + kind, t, lambda: net.mine(base, 0, 0, n), to, cond)
        return act

    def pass_on(*a):
        return sender(net.pass_on, *a)

    def spread(*a, **k):
        return sender(net.spread, *a, **k)

    def z_reduce(base, k0, first_u, first_d, n):
        def climb(t):
            to_up = lambda t: z < 3 - mode(base, t)
            if_(t, lambda t: (z > 0) & (z <= 3 - mode(base, t)), add(base, ZU, t, first_u, n, dn))
            if_(t, to_up, pass_on(base, ZU, t, first_u, n, up, to_up))

        def sink(t):
            to_dn = lambda t: z > mode(base, t)
            if_(t, lambda t: (z < 3) & (z >= mode(base, t)), add(base, ZD, t, first_d, n, up))
            if_(t, to_dn, pass_on(base, ZD, t, first_d, n, dn, to_dn))

        stage(k0 + z, climb)
        stage(k0 + 3 - z, sink)
        if base == OC:
            f = jnp.where(z >= 2, first_u, first_d)
            give = lambda t: side() & (mode(base, t) == 1)
            stage(k0, lambda t: if_(t, give, pass_on(base, W, t, f, n, cross, give)))
            stage(k0 + 1, lambda t: if_(t, lambda t: ~side() & (mode(base, t) == 1), add(base, W, t, f, n, cross)))

    def z_gather(base, k0, first_u, first_d, n):
        own = base == OA

        def sink(t):
            to_dn = lambda t: (z > 0) & (z <= (2 if own else 3 - mode(base, t)))
            if_(t, lambda t: z < 3 - mode(base, t), got(base, GZU, t, first_u, n, up))
            if own:
                top = lambda t: z == 3
                if_(t, top, spread(base, GZU, t, first_u, n, dn, top, own=True))
            if_(t, to_dn, spread(base, GZU, t, first_u, n, dn, to_dn))

        def climb(t):
            to_up = lambda t: (z < 3) & (z >= (1 if own else mode(base, t)))
            if_(t, lambda t: z > mode(base, t), got(base, GZD, t, first_d, n, dn))
            if own:
                bottom = lambda t: z == 0
                if_(t, bottom, spread(base, GZD, t, first_d, n, up, bottom, own=True))
            if_(t, to_up, spread(base, GZD, t, first_d, n, up, to_up))

        stage(k0 + 3 - z, sink)
        stage(k0 + z, climb)
        if base == OC:
            f = jnp.where(z >= 2, first_u, first_d)
            give = lambda t: ~side() & (mode(base, t) == 1)
            stage(k0 + 1, lambda t: if_(t, give, spread(base, GW, t, f, n, cross, give)))
            stage(k0 + 2, lambda t: if_(t, lambda t: side() & (mode(base, t) == 1), got(base, GW, t, f, n, cross)))

    own_a, own_b, own_c = 4 * x + 2 * y + d, 4 * y + 2 * d + x, 4 * d + 2 * x + y

    def kept(t):
        for i, (base, first) in enumerate(((OA, own_a), (OB, own_b), (OC, own_c))):
            if_(t, owner(base), net.keep(i, base, t, first).wait)

    def k1(t):
        net.pass_on(OA, X, t, 4 * (1 - x), 4, xn)
        net.pass_on(OB, Y, t, 4 * (1 - y), 4, yn)

    def k2(t):
        net.add(OA, X, t, 4 * x, 4, xn)
        net.pass_on(OA, Y, t, 4 * x + 2 * (1 - y), 2, yn)
        net.add(OB, Y, t, 4 * y, 4, yn)

    def k4(t):
        if_(t, owner(OC), pass_on(OC, X, t, 4 * d + 2 * (1 - x), 2, xn, owner(OC)))

    def k5(t):
        if_(t, owner(OC), add(OC, X, t, 4 * d + 2 * x, 2, xn),
            pass_on(OC, Y, t, 4 * d + 2 * x + 1 - y, 1, yn, owner(OC)))
        if_(t, owner(OB), pass_on(OB, X, t, 4 * y + 2 * d + 1 - x, 1, xn, owner(OB)))

    def k6(t):
        if_(t, owner(OC), add(OC, Y, t, own_c, 1, yn), net.keep(2, OC, t, own_c).start,
            spread(OC, GY, t, own_c, 1, yn, owner(OC), own=True))
        if_(t, owner(OB), add(OB, X, t, own_b, 1, xn), net.keep(1, OB, t, own_b).start,
            spread(OB, GX, t, own_b, 1, xn, owner(OB), own=True))

    def k7(t):
        if_(t, owner(OC), got(OC, GY, t, 4 * d + 2 * x + 1 - y, 1, yn), spread(OC, GX, t, 4 * d + 2 * x, 2, xn, owner(OC)))
        if_(t, owner(OB), got(OB, GX, t, 4 * y + 2 * d + 1 - x, 1, xn))

    def k10(t):
        net.spread(OB, GY, t, 4 * y, 4, yn)
        net.got(OA, GY, t, 4 * x + 2 * (1 - y), 2, yn)
        net.spread(OA, GX, t, 4 * x, 4, xn)

    def k11(t):
        net.got(OB, GY, t, 4 * (1 - y), 4, yn)
        net.got(OA, GX, t, 4 * (1 - x), 4, xn)
        triple = net.out.at[net.core, t]
        net.send(DONE, t, triple, triple, cn, lambda: net.part.at[0])

    def k12(t):
        other = net.out.at[1 - net.core, t]
        net.copy(DONE, t, other, other, cn).wait_recv()

    stage(7, kept)
    stage(1, k1)
    z_reduce(OC, 1, 4, 0, 4)
    compute(0)
    stage(2, k2)
    z_reduce(OB, 2, 4 * y + 2, 4 * y, 2)
    stage(3, lambda t: net.add(OA, Y, t, 4 * x + 2 * y, 2, yn))
    z_reduce(OA, 3, 4 * x + 2 * y + 1, 4 * x + 2 * y, 1)
    stage(4, k4)
    stage(5, k5)
    compute(1)
    stage(6, k6)
    stage(6, lambda t: if_(t, owner(OA), net.keep(0, OA, t, own_a).start))
    z_gather(OA, 6, 4 * x + 2 * y + 1, 4 * x + 2 * y, 1)
    stage(7, k7)
    z_gather(OB, 7, 4 * y + 2, 4 * y, 2)
    stage(8, lambda t: if_(t, owner(OC), got(OC, GX, t, 4 * d + 2 * (1 - x), 2, xn)))
    z_gather(OC, 8, 4, 0, 4)
    compute(2)
    stage(9, lambda t: net.spread(OA, GY, t, 4 * x + 2 * y, 2, yn))
    stage(10, k10)
    stage(11, k11)
    stage(14, momentum.stored)
    stage(12, k12)
    stage(12, momentum.load)
    stage(13, momentum.update)


def exchange_kernel(scale, x_ref, y_ref, w1_ref, w2_ref, m1_ref, m2_ref, out_ref, m1_new, m2_new, h_ref, low_ref, turn_ref, saved_ref, w1_st, w2_st, gbuf, cslot, part,
                    tile1, tile2, grads, wsem, psem, msem, ssem, rsem, csem, ksem, *slots):
    net = Net(part, out_ref, dict(zip(SLOT_ROWS, slots)), ssem, rsem, csem, ksem)
    core = net.core
    momentum = Momentum(out_ref, (m1_ref, m2_ref), (m1_new, m2_new), (tile1, tile2), grads, msem)

    half = F // 2

    def weights(i):
        b, cols = lax.rem(i, 4), pl.ds(pl.multiple_of(lax.rem(i, 2) * half, half), half)
        return (pltpu.make_async_copy(w1_ref.at[i // 2, :, cols], w1_st.at[b], wsem.at[0, b]),
                pltpu.make_async_copy(w2_ref.at[i // 2, cols, :], w2_st.at[b], wsem.at[1, b]))

    def load(i):
        for c in weights(i):
            c.start()

    def loaded(i):
        for c in weights(i):
            c.wait()

    net.greet()
    for i in range(3):
        load(i)
    h_ref[...] = x_ref[...].astype(F32)

    @pl.loop(0, 2 * L)
    def _(i):
        pl.when(i < 2 * L - 3)(lambda: load(i + 3))
        l, b = i // 2, lax.rem(i, 4)

        @pl.when(lax.rem(i, 2) == 0)
        def _():
            saved_ref[l] = h_ref[...].astype(BF)
        loaded(i)
        act = gelu(dot(saved_ref[l], w1_st[b].astype(BF))).astype(BF)
        h_ref[...] = h_ref[...] + dot(act, w2_st[b].astype(BF))

    h_ref[...] = (h_ref[...] - y_ref[...].astype(F32)) * scale

    def backward(t, i):
        c = 3 * t + i
        l, j = L - 1 - c // TPL, lax.rem(c, TPL)
        i0 = 2 * l
        b, col = lax.rem(i0 + j // (TPL // 2), 4), pl.multiple_of(lax.rem(j, TPL // 2) * FT, FT)

        def piece(l):
            i = 2 * l + j // (TPL // 2)
            b, to = lax.rem(i, 4), pl.ds(col, FT)
            frm = pl.ds(pl.multiple_of(j * FT, FT), FT)
            return (pltpu.make_async_copy(w1_ref.at[l, :, frm], w1_st.at[b, :, to], psem.at[0, lax.rem(l, 2), j]),
                    pltpu.make_async_copy(w2_ref.at[l, frm, :], w2_st.at[b, to, :], psem.at[1, lax.rem(l, 2), j]))

        @pl.when((l < L - 1) & (l > 0))
        def _():
            for p in piece(l - 1):
                p.start()

        @pl.when(l < L - 2)
        def _():
            for p in piece(l):
                p.wait()

        @pl.when(j == 0)
        def _():
            low_ref[...] = h_ref[...].astype(BF)
            turn_ref[...] = saved_ref[l].T

        h_low, g_low = saved_ref[l], low_ref[...]
        w1 = w1_st[b, :, pl.ds(col, FT)].astype(BF)
        w2 = w2_st[b, pl.ds(col, FT), :].astype(BF)
        act, slope = gelu_both(dot(h_low, w1))
        q = (slope * dot(g_low, w2, 1, 1)).astype(BF)
        g2 = dot(act.astype(BF), g_low, 0, 0).astype(BF)
        g1 = dot(turn_ref[...], q).astype(BF)
        k, row = lax.rem(t, 2), i * (TR // 3)
        for half in range(FT // LN):
            gbuf[k, 0, pl.ds(row + half * D, D)] = g1[:, half * LN:(half + 1) * LN]
        for q4 in range(D // LN):
            gbuf[k, 1, pl.ds(row + q4 * FT, FT)] = g2[:, q4 * LN:(q4 + 1) * LN]
        h_ref[...] = h_ref[...] + dot(q, w1, 1, 1)

    def core_copy(t):
        return net.copy(CORE, t, gbuf.at[lax.rem(t, 2), 1 - core], net_slot(t), net.cn)

    def net_slot(t):
        return cslot.at[lax.rem(t, SLOTS)]

    def core_add(t):
        core_copy(t).wait_send()
        net.copy(CORE, t, net_slot(t), net_slot(t), net.cn).wait_recv()
        part[lax.rem(t, RING)] = gbuf[lax.rem(t, 2), core] + cslot[lax.rem(t, SLOTS)]

    net.greeted()

    @pl.loop(0, NT + DEPTH)
    def _(s):
        pl.when(s >= LAG)(net.take_credit)
        pl.when(valid(s - 1))(lambda: core_add(s - 1))
        def compute(i):
            @pl.when(valid(s))
            def _():
                backward(s, i)
                if i == 2:
                    core_copy(s).start()

        pump(net, s, compute, momentum)
        net.give_credit()

    net.all_sent()
    for _ in range(LAG):
        net.take_credit()


def exchange(x_now, y_now, w_first, w_second, m_first, m_second, scale):
    vm = pl.BlockSpec(memory_space=pltpu.VMEM)
    hbm = pl.BlockSpec(memory_space=pl.ANY)
    return pl.pallas_call(
        functools.partial(exchange_kernel, scale),
        out_shape=[jax.ShapeDtypeStruct((2, NT, TR, LN), BF), jax.ShapeDtypeStruct((L, D, F), F32),
                   jax.ShapeDtypeStruct((L, F, D), F32)],
        in_specs=[vm, vm] + [hbm] * 4,
        out_specs=[hbm] * 3,
        scratch_shapes=[
            pltpu.VMEM((R, D), F32), pltpu.VMEM((R, D), BF), pltpu.VMEM((D, R), BF), pltpu.VMEM((L, R, D), BF),
            pltpu.VMEM((4, D, F // 2), F32), pltpu.VMEM((4, F // 2, D), F32),
            pltpu.VMEM((2, 2, TR, LN), BF), pltpu.VMEM((SLOTS, TR, LN), BF), pltpu.VMEM((RING, TR, LN), BF),
            pltpu.VMEM((2, 3, D, FT), F32), pltpu.VMEM((2, 3, FT, D), F32), pltpu.VMEM((2, 2, TR, LN), BF),
            pltpu.SemaphoreType.DMA((2, 4)), pltpu.SemaphoreType.DMA((2, 2, TPL)), pltpu.SemaphoreType.DMA((3, 2, 2, 3)), pltpu.SemaphoreType.DMA((NTYPE, SLOTS)), pltpu.SemaphoreType.DMA((NTYPE, SLOTS)),
            pltpu.SemaphoreType.REGULAR((5,)), pltpu.SemaphoreType.DMA((3,)),
        ] + [pltpu.VMEM((SLOTS, n, LN), BF) for n in SLOT_ROWS.values()],
        compiler_params=pltpu.CompilerParams(collective_id=0, has_side_effects=True, vmem_limit_bytes=63 * 2**20),
        name="exchange",
    )(x_now, y_now, w_first, w_second, m_first, m_second)


UT = 512
TILES = F // UT
BUFS, AHEAD = 8, 4


def update_kernel(rate, x_ref, w1_ref, w2_ref, m1_ref, m2_ref, w1o, w2o, m1o, m2o, h_ref, low_ref, w1, w2, m1, m2, isem, osem):
    olds, news, tiles = (w1_ref, w2_ref, m1_ref, m2_ref), (w1o, w2o, m1o, m2o), (w1, w2, m1, m2)

    def copy(a, i, back):
        l, cols = i // TILES, pl.ds(pl.multiple_of(lax.rem(i, TILES) * UT, UT), UT)
        where = (l, slice(None), cols) if a % 2 == 0 else (l, cols)
        k = lax.rem(i, BUFS)
        if back:
            return pltpu.make_async_copy(tiles[a].at[k], news[a].at[where], osem.at[a, k])
        return pltpu.make_async_copy(olds[a].at[where], tiles[a].at[k], isem.at[a, k])

    def load(i):
        for a in range(4):
            copy(a, i, False).start()

    def stored(i):
        for a in range(4):
            copy(a, i, True).wait()

    for i in range(AHEAD):
        load(i)
    h_ref[...] = x_ref[...].astype(F32)

    @pl.loop(0, L * TILES)
    def _(i):
        pl.when(i + AHEAD >= BUFS)(lambda: pl.when(i + AHEAD < L * TILES)(lambda: stored(i + AHEAD - BUFS)))
        pl.when(i + AHEAD < L * TILES)(lambda: load(i + AHEAD))

        @pl.when(lax.rem(i, TILES) == 0)
        def _():
            low_ref[...] = h_ref[...].astype(BF)

        for a in range(4):
            copy(a, i, False).wait()
        for a in (2, 3):
            copy(a, i, True).start()
        k = lax.rem(i, BUFS)
        first = w1[k] - rate * m1[k]
        w1[k] = first
        copy(0, i, True).start()
        act = gelu(dot(low_ref[...], first.astype(BF))).astype(BF)
        second = w2[k] - rate * m2[k]
        w2[k] = second
        copy(1, i, True).start()
        h_ref[...] = h_ref[...] + dot(act, second.astype(BF))

    @pl.loop(L * TILES - BUFS, L * TILES)
    def _(i):
        stored(i)


def update(x_next, w_first, w_second, m_first, m_second, rate):
    vm = pl.BlockSpec(memory_space=pltpu.VMEM)
    hbm = pl.BlockSpec(memory_space=pl.ANY)
    return pl.pallas_call(
        functools.partial(update_kernel, rate),
        in_specs=[vm] + [hbm] * 4,
        out_specs=[hbm] * 4 + [vm],
        out_shape=[jax.ShapeDtypeStruct((L, D, F), F32), jax.ShapeDtypeStruct((L, F, D), F32)] * 2
        + [jax.ShapeDtypeStruct((R, D), F32)],
        scratch_shapes=[pltpu.VMEM((R, D), BF)] + [pltpu.VMEM((BUFS, D, UT), F32), pltpu.VMEM((BUFS, UT, D), F32)] * 2
        + [pltpu.SemaphoreType.DMA((4, BUFS))] * 2,
        compiler_params=pltpu.CompilerParams(vmem_limit_bytes=60 * 2**20),
        cost_estimate=pl.CostEstimate(flops=4 * L * R * D * F, bytes_accessed=16 * 2 * L * D * F, transcendentals=L * R * F),
        name="update",
    )(x_next, w_first, w_second, m_first, m_second)


def solution(mesh):
    rows_spec = P(("pod", "data"), None)
    full_spec = P()
    devices = mesh.shape["pod"] * mesh.shape["data"]

    def train_step(w_first, w_second, m_first, m_second, x_now, y_now, x_next, y_next):
        scale = 1.0 / (x_now.shape[0] * devices * D)
        _, m_first, m_second = exchange(x_now, y_now, w_first, w_second, m_first, m_second, scale)
        w1, w2, m1, m2, hidden = update(x_next, w_first, w_second, m_first, m_second, LEARN_BASE / L)
        resid = hidden - y_next.astype(F32)
        loss = jnp.sum(resid * resid, axis=-1) / (2 * D)
        return w1, w2, m1, m2, loss, hidden

    return jax.shard_map(train_step, mesh=mesh, in_specs=(full_spec,) * 4 + (rows_spec,) * 4,
                         out_specs=(full_spec,) * 4 + (P(("pod", "data")), rows_spec), check_vma=False)
```
